128 devices in a mesh: dp: 16 (over y, x), tensor: 8 (over z, core).
Axes of the slice: x: 4, y: 4, z: 4, core: 2. Of those that a mesh axis runs over, the one named last changes fastest.
Arguments:
- tokens: bfloat16 [8192, 3584], P('dp'), may hold values from -6 to 6
- gate_weight: bfloat16 [3584, 10240], P(None, 'tensor'), may hold values from -0.09375 to 0.09375
- up_act: bfloat16 [8192, 10240], P('dp', 'tensor'), may hold values from -6 to 6
- hidden_cot: bfloat16 [8192, 10240], P('dp', 'tensor'), may hold values from -6 to 6
- lag_grads: bfloat16 [16, 3584, 10240], P('dp', None, 'tensor'), may hold values from -8 to 8, as said below
- skip_mask: int32 [16], P('dp'), may hold values 0 or 1
- aggregate: float32 [3584, 10240], P('dp', 'tensor'), may hold values from -3 to 3
Outputs:
- new_aggregate: float32 [3584, 10240], P('dp', 'tensor')
- input_grad: bfloat16 [8192, 3584], P('dp', 'tensor')
- change_rms: float32 [16], P('dp')
The draws below stay inside these ranges and needn't reach their ends.
Inputs may be any that keep to these rules, and one draw needn't show every extreme that they name: `lag_grads`: real-valued.
All inputs are finite; a program needn't handle non-finite values. No bound on the sum of `skip_mask` on one device may be relied on, other than what follows from the above.
Results may differ from the reference program's by a relative error of at most 0.014.
Values may be sent and summed in bfloat16 or wider, within the bound.
No kernel may reach another device: no remote copies, remote signals or barrier semaphores. Data moves between devices by JAX's collectives and lax.ppermute only.
A program may use at most 128 MiB of HBM per device.

```python
import jax
import jax.numpy as jnp
from jax import lax

D = 3584
FF = 10240
TOK_DEV = 512
TOKENS = 8192
N_DP = 16


def draw_lag_grads(key, part):
    keys = jax.random.split(jax.random.fold_in(key, 17), 4)
    worker = jnp.arange(N_DP).astype(jnp.float32)
    wscale = 0.03 * 10.0 ** ((worker + jax.random.uniform(keys[0], (N_DP,))) / N_DP)
    rowscale = jnp.exp(jax.random.uniform(keys[1], (D,)) * jnp.log(10.0))
    position = jnp.arange(FF).astype(jnp.float32) / FF
    colscale = jnp.exp(jax.random.uniform(keys[2], (FF,)) * jnp.log(10.0)) * 3.0 ** position
    noise = jnp.clip(jax.random.normal(keys[3], (N_DP, D, FF)), -5.0, 5.0)
    norm = 41.0
    values = noise * wscale[:, None, None] * rowscale[None, :, None] * colscale[None, None, :] / norm
    return jnp.clip(values, -8.0, 8.0).astype(jnp.bfloat16)


def plant(entries, own_key, smallest, high):
    place = [jax.random.randint(jax.random.fold_in(own_key, axis), (), 0, length) for axis, length in enumerate(entries.shape)]
    longest = entries.shape.index(max(entries.shape))
    beside = place[:longest] + [(place[longest] + 1) % entries.shape[longest]] + place[longest + 1:]
    return entries.at[tuple(place)].set(smallest).at[tuple(beside)].set(high)


def level_of(key, shape, cuts, least, top_value):
    def one(axis_at, parts):
        draws = jax.random.uniform(jax.random.fold_in(jax.random.fold_in(key, 6), axis_at), (parts,), jnp.float32, least / len(cuts), top_value / len(cuts))
        return jnp.repeat(jnp.exp(draws), shape[axis_at] // parts).reshape((-1,) + (1,) * (len(shape) - axis_at - 1))

    level = one(*cuts[0])
    for cut in cuts[1:]:
        level = level * one(*cut)
    return level


def centred(key, extent, scale, most, pieces=(), kind=jnp.bfloat16):
    gain = level_of(key, extent, pieces, -0.22, 0.18) if pieces else 1.0
    array = jax.random.normal(key, extent, jnp.float32) * scale * gain
    return jnp.minimum(jnp.maximum(array, -most), most).astype(kind)


def setup_inputs(seed: int = 0) -> dict:
    key_list = jax.random.split(jax.random.key(seed), 8)
    return {
        "tokens": centred(key_list[0], (TOKENS, D), 1.0, 6.0, ((0, 16),)),
        "gate_weight": centred(key_list[1], (D, FF), D ** -0.5, 0.09375, ((1, 8),)),
        "up_act": centred(key_list[2], (TOKENS, FF), 1.0, 6.0, ((0, 16), (1, 8))),
        "hidden_cot": centred(key_list[3], (TOKENS, FF), 1.0, 6.0, ((0, 16), (1, 8))),
        "lag_grads": draw_lag_grads(jax.random.fold_in(key_list[7], 71), 0),
        "skip_mask": plant((jax.random.randint(key_list[5], (N_DP,), 0, 2) < 1).astype(jnp.int32), jax.random.fold_in(key_list[5], 1), 0, 1),
        "aggregate": centred(key_list[6], (D, FF), 0.2, 3.0, ((0, 16), (1, 8)), jnp.float32),
    }


clip_level = 0.1

def reference(tokens, gate_weight, up_act, hidden_cot, lag_grads, skip_mask, aggregate):
    gate = jnp.dot(tokens, gate_weight, preferred_element_type=jnp.float32)
    sig = jax.nn.sigmoid(gate)
    d_gate = (hidden_cot.astype(jnp.float32) * up_act.astype(jnp.float32) * sig * (1.0 + gate * (1.0 - sig))).astype(jnp.bfloat16)
    input_grad = jnp.dot(d_gate, gate_weight.T, preferred_element_type=jnp.float32).astype(jnp.bfloat16)
    worker_tokens = tokens.reshape(N_DP, TOK_DEV, D)
    worker_dgate = d_gate.reshape(N_DP, TOK_DEV, FF)
    inverse = 1.0 / TOK_DEV

    def one_worker(total, item):
        x_rows, d_rows, lag, flag = item
        grad = lax.dot_general(x_rows, d_rows, (((0,), (0,)), ((), ())), preferred_element_type=jnp.float32) * inverse
        change = grad - lag.astype(jnp.float32)
        rms = jnp.sqrt(jnp.sum(change * change) / (D * FF) + 1e-06)
        factor = flag.astype(jnp.float32) * jnp.minimum(1.0, clip_level / rms)
        sent = (factor * change).astype(jnp.bfloat16).astype(jnp.float32)
        return (total + sent, rms)
    new_aggregate, change_rms = lax.scan(one_worker, aggregate, (worker_tokens, worker_dgate, lag_grads, skip_mask))
    return (new_aggregate, input_grad, change_rms)
```

```python
import functools

import jax
import jax.numpy as jnp
from jax import lax
from jax.experimental import pallas as pl
from jax.experimental.pallas import tpu as pltpu
from jax.sharding import Mesh
from jax.sharding import PartitionSpec as P

D = 3584
FF = 10240
TOK = 512
COLS = 1280
HALF = 640
BLK = 224
SUB = 112
INB = 448
CLIP = 0.1
TENSOR = ("z", "c")
EVEN = [(0, 1), (1, 0), (2, 3), (3, 2)]
ODD = [(1, 2), (2, 1), (3, 0), (0, 3)]
VMEM_LIMIT = 60 * 1024 * 1024


def cost(flops, nbytes):
    return pl.CostEstimate(flops=flops, bytes_accessed=nbytes, transcendentals=0)


def gate_kernel(x_ref, w_ref, up_ref, hc_ref, dg_ref, xt_ref):
    j = pl.program_id(0)
    gate = jnp.dot(x_ref[...], w_ref[...], preferred_element_type=jnp.float32)
    sig = 1.0 / (1.0 + jnp.exp(-gate))
    dg_ref[...] = (
        hc_ref[...].astype(jnp.float32)
        * up_ref[...].astype(jnp.float32)
        * sig
        * (1.0 + gate * (1.0 - sig))
    ).astype(jnp.bfloat16)
    start = pl.multiple_of(jnp.minimum(j * 768, D - 768), 128)
    xt_ref[pl.ds(start, 768), :] = x_ref[:, pl.ds(start, 768)].T


def gates(x, w, up, hc):
    return pl.pallas_call(
        gate_kernel,
        grid=(5,),
        in_specs=[
            pl.BlockSpec((TOK, D), lambda j: (0, 0)),
            pl.BlockSpec((D, 256), lambda j: (0, j)),
            pl.BlockSpec((TOK, 256), lambda j: (0, j)),
            pl.BlockSpec((TOK, 256), lambda j: (0, j)),
        ],
        out_specs=[
            pl.BlockSpec((TOK, 256), lambda j: (0, j)),
            pl.BlockSpec((D, TOK), lambda j: (0, 0)),
        ],
        out_shape=[
            jax.ShapeDtypeStruct((TOK, COLS), jnp.bfloat16),
            jax.ShapeDtypeStruct((D, TOK), jnp.bfloat16),
        ],
        compiler_params=pltpu.CompilerParams(
            vmem_limit_bytes=VMEM_LIMIT, dimension_semantics=("arbitrary",)
        ),
        cost_estimate=cost(2 * TOK * D * COLS, 20_000_000),
        name="gates",
    )(x, w, up, hc)


def grad_kernel(steps, tbl, dg_ref, xt_hbm, lag_hbm, *rest):
    n = len(steps)
    outs, ss_ref = rest[: 2 * n], rest[2 * n]
    xt_s, lag_s, stage, sem_x, sem_l, sem_o = rest[2 * n + 1 :]

    def loads(s):
        g = steps[s]
        made = []
        for m in range(4):
            row = pl.multiple_of(tbl[4 * s + m] * BLK, 16)
            made.append(
                pltpu.make_async_copy(
                    xt_hbm.at[pl.ds(row, BLK), :], xt_s.at[s, m], sem_x.at[s, m]
                )
            )
            made.append(
                pltpu.make_async_copy(
                    lag_hbm.at[pl.ds(row, BLK), pl.ds(g * HALF, HALF)],
                    lag_s.at[s, m],
                    sem_l.at[s, m],
                )
            )
        return made

    def stores(s):
        return [
            pltpu.make_async_copy(stage.at[s, h], outs[2 * s + h], sem_o.at[s, h])
            for h in range(2)
        ]

    for s in range(n):
        for copy in loads(s):
            copy.start()
    ss_ref[...] = jnp.zeros_like(ss_ref)
    for s in range(n):
        for copy in loads(s):
            copy.wait()
        g = steps[s]
        lhs = xt_s[s].reshape(4 * BLK, TOK)
        change = jnp.dot(
            lhs, dg_ref[:, g * HALF : (g + 1) * HALF], preferred_element_type=jnp.float32
        ) * (1.0 / TOK) - lag_s[s].reshape(4 * BLK, HALF).astype(jnp.float32)
        sq = jnp.sum((change * change).reshape(4 * BLK // 8, 8, HALF), axis=0)
        ss_ref[...] += (
            sq[:, 0:128] + sq[:, 128:256] + sq[:, 256:384] + sq[:, 384:512] + sq[:, 512:640]
        )
        out = change.astype(jnp.bfloat16).reshape(4, BLK, HALF)
        stage[s, 0] = out[:, :SUB]
        stage[s, 1] = out[:, SUB:]
        for copy in stores(s):
            copy.start()
    for s in range(n):
        for copy in stores(s):
            copy.wait()


def grads(steps, table, dg, xt, lag, name):
    n = len(steps)
    anyspec = pl.BlockSpec(memory_space=pl.ANY)
    vmem = pl.BlockSpec(memory_space=pltpu.VMEM)
    return pl.pallas_call(
        functools.partial(grad_kernel, steps),
        in_specs=[pl.BlockSpec(memory_space=pltpu.SMEM), vmem, anyspec, anyspec],
        out_specs=[anyspec] * (2 * n) + [vmem],
        out_shape=[jax.ShapeDtypeStruct((4, SUB, HALF), jnp.bfloat16)] * (2 * n)
        + [jax.ShapeDtypeStruct((8, 128), jnp.float32)],
        scratch_shapes=[
            pltpu.VMEM((n, 4, BLK, TOK), jnp.bfloat16),
            pltpu.VMEM((n, 4, BLK, HALF), jnp.bfloat16),
            pltpu.VMEM((n, 2, 4, SUB, HALF), jnp.bfloat16),
            pltpu.SemaphoreType.DMA((n, 4)),
            pltpu.SemaphoreType.DMA((n, 4)),
            pltpu.SemaphoreType.DMA((n, 2)),
        ],
        compiler_params=pltpu.CompilerParams(vmem_limit_bytes=VMEM_LIMIT),
        cost_estimate=cost(2 * TOK * 896 * HALF * n, 4_000_000 * n),
        name=name,
    )(table, dg, xt, lag)


def input_kernel(tbl, w_ref, dg_ref, *refs):
    i = pl.program_id(0)
    part = lax.dot_general(
        w_ref[...], dg_ref[...], (((1,), (1,)), ((), ())), preferred_element_type=jnp.float32
    )
    if len(refs) == 1:
        refs[0][0] = part.astype(jnp.bfloat16)
    else:
        total = (part + refs[0][0].astype(jnp.float32)).astype(jnp.bfloat16)
        for pos in range(4):

            @pl.when(i == pos)
            def _():
                refs[1 + pos][...] = total


def inputs(table, w, dg, other=None):
    ins = [
        pl.BlockSpec((INB, COLS), lambda i, t: (t[i], 0)),
        pl.BlockSpec((TOK, COLS), lambda i, t: (0, 0)),
    ]
    each = pl.BlockSpec((1, INB, TOK), lambda i, t: (i, 0, 0))
    if other is None:
        args, outs, shapes = (), each, jax.ShapeDtypeStruct((4, INB, TOK), jnp.bfloat16)
    else:
        ins.append(each)
        args = (other,)
        outs = [pl.BlockSpec((INB, TOK), lambda i, t: (0, 0))] * 4
        shapes = [jax.ShapeDtypeStruct((INB, TOK), jnp.bfloat16)] * 4
    return pl.pallas_call(
        input_kernel,
        grid_spec=pltpu.PrefetchScalarGridSpec(
            num_scalar_prefetch=1, grid=(4,), in_specs=ins, out_specs=outs
        ),
        out_shape=shapes,
        compiler_params=pltpu.CompilerParams(
            vmem_limit_bytes=VMEM_LIMIT, dimension_semantics=("arbitrary",)
        ),
        cost_estimate=cost(2 * TOK * 4 * INB * COLS, 8_000_000),
        name="inputs",
    )(table, w, dg, *args)


def offsets(i):
    sign = 1 - 2 * (i % 2)
    return (i + 2) % 4, (i + sign) % 4, (i - sign) % 4, i


def f32(value):
    return value.astype(jnp.float32)


def body(tokens, gate_weight, up_act, hidden_cot, lag_grads, skip_mask, aggregate):
    y, x = lax.axis_index("y"), lax.axis_index("x")
    z, c = lax.axis_index("z"), lax.axis_index("c")
    place = {"x": offsets(x), "y": offsets(y)}
    axes = (("x", "y"), ("y", "x"))

    def blocks(g, k):
        first, second = axes[g]
        far2, near2, back2, own2 = place[second]
        one = place[first][k]
        result = []
        for two in (near2, far2, back2, own2):
            at = {first: one, second: two}
            result.append(at["y"] * 4 + at["x"])
        return result

    def table(steps):
        flat = [b for g, k in steps for b in blocks(g, k)]
        return jnp.stack(flat).astype(jnp.int32)

    def swap(value, axis, pairs):
        return lax.ppermute(value, axis, pairs)

    lag = lag_grads[0]
    dg, xt = gates(tokens, gate_weight, up_act, hidden_cot)
    relays = ((0, 0), (1, 0))
    rests = ((0, 1), (0, 2), (1, 1), (1, 2), (0, 3), (1, 3))
    *relay, ss0 = grads((0, 1), table(relays), dg, xt, lag, "relay_grads")
    order = ((0, 0), (1, 0), (0, 1), (1, 1))
    pairs = (EVEN, ODD)
    got_relay = {(g, h): swap(relay[2 * g + h], axes[g][0], pairs[h]) for g, h in order}
    *rest, ss1 = grads((0, 0, 1, 1, 0, 1), table(rests), dg, xt, lag, "rest_grads")
    piece = {}
    for s, (g, k) in enumerate(rests):
        for h in range(2):
            piece[g, k, h] = rest[2 * s + h]
    got_near = {
        (g, h): swap(piece[g, 1 + h, h], axes[g][0], pairs[h]) for g, h in order
    }
    total = ss0 + ss1
    total = total + swap(total, "c", [(0, 1), (1, 0)])
    total = total + swap(total, "z", EVEN)
    total = total + swap(total, "z", ODD)
    rms = jnp.sqrt(jnp.sum(total) / (D * FF) + 1e-06)
    factor = f32(skip_mask[0]) * jnp.minimum(1.0, CLIP / rms)
    wide = jnp.broadcast_to(factor, (8, 128))
    theirs = {
        (g, h): swap(wide, axes[g][0], pairs[h])[0, 0] for g, h in order
    }

    zs = jnp.stack([(z + 1) % 4, (z + 3) % 4, (z + 2) % 4, z]).astype(jnp.int32)
    away = inputs(zs * 2 + (1 - c), gate_weight, dg)
    away = swap(away, "c", [(0, 1), (1, 0)])
    up1, down1, two, mine = inputs(zs * 2 + c, gate_weight, dg, away)
    ring = lambda by: [(i, (i + by) % 4) for i in range(4)]
    inp = (
        f32(mine)
        + f32(swap(up1, "z", ring(1)))
        + f32(swap(down1, "z", ring(3)))
        + f32(swap(two, "z", ring(2)))
    ).astype(jnp.bfloat16)

    relayed = {}
    for g, h in order:
        mixed = (
            factor * f32(piece[g, 2 - h, h]) + theirs[g, h] * f32(got_relay[g, h])
        ).astype(jnp.bfloat16)
        relayed[g, h] = swap(mixed, axes[g][0], pairs[1 - h])

    def merged(g, h, lo, hi):
        return (
            factor * f32(piece[g, 3, h][lo:hi])
            + theirs[g, h] * f32(got_near[g, h][lo:hi])
            + f32(relayed[g, h][lo:hi])
        )

    third = {
        (g, h): swap(merged(g, h, h, 2 + h).astype(jnp.bfloat16), axes[g][1], pairs[h])
        for g, h in order
    }
    fourth = {}
    for g, h in order:
        back = 2 - 2 * h
        value = merged(g, h, back, back + 1) + f32(third[g, h][1 - h : 2 - h])
        fourth[g, h] = swap(value.astype(jnp.bfloat16), axes[g][1], pairs[1 - h])
    rows = []
    for h in range(2):
        cols = [
            merged(g, h, 3, 4)[0] + f32(third[g, h][h]) + f32(fourth[g, h][0])
            for g in range(2)
        ]
        rows.append(jnp.concatenate(cols, axis=1))
    new = aggregate + jnp.concatenate(rows, axis=0)
    return new, inp.T, rms.reshape(1)


def solution(mesh):
    finer = Mesh(mesh.devices.reshape(4, 4, 4, 2), ("y", "x", "z", "c"))
    dp = ("y", "x")
    placed = (
        P(dp, None),
        P(None, TENSOR),
        P(dp, TENSOR),
        P(dp, TENSOR),
        P(dp, None, TENSOR),
        P(dp),
        P(dp, TENSOR),
    )
    return jax.shard_map(
        body,
        mesh=finer,
        in_specs=placed,
        out_specs=(P(dp, TENSOR), P(dp, TENSOR), P(dp)),
        check_vma=False,
    )
```

```python
import jax
import jax.numpy as jnp
from jax import lax
from jax.experimental import pallas as pl
from jax.experimental.pallas import tpu as pltpu
from jax.sharding import Mesh
from jax.sharding import PartitionSpec as P

D = 3584
FF = 10240
TOK = 512
COLS = 1280
HALF = 640
CHUNK = 256
BLK = 224
SUB = 112
INB = 448
CLIP = 0.1
MIB = 1024 * 1024
TENSOR = ("z", "c")
EVEN = [(0, 1), (1, 0), (2, 3), (3, 2)]
ODD = [(1, 2), (2, 1), (3, 0), (0, 3)]
PAIRS = (EVEN, ODD)
AXES = (("x", "y"), ("y", "x"))
PARTS = ((0, 0), (1, 0), (0, 1), (1, 1))

HBM = pl.BlockSpec(memory_space=pltpu.HBM)
VMEM = pl.BlockSpec(memory_space=pltpu.VMEM)
SMEM = pl.BlockSpec(memory_space=pltpu.SMEM)


def f32(value):
    return value.astype(jnp.float32)


def bf16(value):
    return value.astype(jnp.bfloat16)


def shape(*dims, dtype=jnp.bfloat16):
    return jax.ShapeDtypeStruct(dims, dtype)


def cost(flops, nbytes):
    return pl.CostEstimate(flops=flops, bytes_accessed=nbytes, transcendentals=0)


def offsets(i):
    sign = 1 - 2 * (i % 2)
    return (i + 2) % 4, (i + sign) % 4, (i - sign + 4) % 4, i


def blocks(g, k):
    place = {"x": offsets(lax.axis_index("x")), "y": offsets(lax.axis_index("y"))}
    first, second = AXES[g]
    one = place[first][k]
    far, near, back, own = place[second]
    result = []
    for two in (near, far, back, own):
        at = {first: one, second: two}
        result.append(at["y"] * 4 + at["x"])
    return result


def change_of(g, k, dg_ref, xt_ref, lag_ref, ss_ref, outs):
    rows = [pl.multiple_of(b * BLK, 32) for b in blocks(g, k)]
    lhs = jnp.concatenate([xt_ref[pl.ds(row, BLK), :] for row in rows], axis=0)
    cols = slice(g * HALF, (g + 1) * HALF)
    grad = jnp.dot(lhs, dg_ref[:, cols], preferred_element_type=jnp.float32)
    for m, row in enumerate(rows):
        change = grad[m * BLK : (m + 1) * BLK] * (1.0 / TOK) - f32(
            lag_ref[pl.ds(row, BLK), cols]
        )
        sq = jnp.sum((change * change).reshape(BLK // 8, 8, HALF), axis=0)
        ss_ref[...] += sum(sq[:, i * 128 : (i + 1) * 128] for i in range(5))
        out = bf16(change)
        outs[0][m] = out[:SUB]
        outs[1][m] = out[SUB:]


def first_kernel(
    x_hbm, w_hbm, up_hbm, hc_hbm, lag_hbm,
    dg_ref, xt_ref, w_ref, lag_ref, r00, r01, r10, r11, ss_ref,
    x_s, up_s, hc_s, gate_s, sem_x, sem_w, sem_a, sem_l,
):
    nw = COLS // CHUNK
    wide = [pl.ds(j * CHUNK, CHUNK) for j in range(nw)]
    get_x = pltpu.make_async_copy(x_hbm, x_s, sem_x.at[0])
    get_w = [
        pltpu.make_async_copy(w_hbm.at[:, wide[j]], w_ref.at[:, wide[j]], sem_w.at[j])
        for j in range(nw)
    ]
    get_up = pltpu.make_async_copy(up_hbm, up_s, sem_a.at[0])
    get_hc = pltpu.make_async_copy(hc_hbm, hc_s, sem_a.at[1])
    relays = blocks(0, 0) + blocks(1, 0)[:1] + blocks(1, 0)[2:]
    get_lag = []
    for b in relays + [b for k in (1, 2, 3) for i, b in enumerate(blocks(0, k)) if i != 1]:
        at = pl.ds(pl.multiple_of(b * BLK, 32), BLK)
        get_lag.append(
            pltpu.make_async_copy(lag_hbm.at[at, :], lag_ref.at[at, :], sem_l.at[len(get_lag)])
        )
    get_x.start()
    get_w[0].start()
    get_up.start()
    get_hc.start()
    for copy in get_w[1:]:
        copy.start()
    for copy in get_lag:
        copy.start()
    get_x.wait()
    for j in range(nw):
        get_w[j].wait()
        at = wide[j]
        gate = jnp.dot(x_s[...], w_ref[:, at], preferred_element_type=jnp.float32)
        lo, hi = j * 768, min(D, j * 768 + 768)
        xt_ref[lo:hi, :] = x_s[:, lo:hi].T
        if j == 0:
            get_up.wait()
            get_hc.wait()
        sig = 1.0 / (1.0 + jnp.exp(-gate))
        dg_ref[:, at] = bf16(
            f32(hc_s[:, at]) * f32(up_s[:, at]) * sig * (1.0 + gate * (1.0 - sig))
        )
    ss_ref[...] = jnp.zeros_like(ss_ref)
    for copy in get_lag[:7]:
        copy.wait()
    change_of(0, 0, dg_ref, xt_ref, lag_ref, ss_ref, (r00, r01))
    change_of(1, 0, dg_ref, xt_ref, lag_ref, ss_ref, (r10, r11))
    for copy in get_lag[7:]:
        copy.wait()


PIECE = (4, SUB, HALF)


def first(x, w, up, hc, lag):
    return pl.pallas_call(
        first_kernel,
        in_specs=[HBM] * 5,
        out_specs=[VMEM] * 9,
        out_shape=[shape(TOK, COLS), shape(D, TOK), shape(D, COLS), shape(D, COLS)]
        + [shape(*PIECE)] * 4
        + [shape(8, 128, dtype=jnp.float32)],
        scratch_shapes=[
            pltpu.VMEM((TOK, D), jnp.bfloat16),
            pltpu.VMEM((TOK, COLS), jnp.bfloat16),
            pltpu.VMEM((TOK, COLS), jnp.bfloat16),
            pltpu.VMEM((8, 128), jnp.float32),
            pltpu.SemaphoreType.DMA((1,)),
            pltpu.SemaphoreType.DMA((COLS // CHUNK,)),
            pltpu.SemaphoreType.DMA((2,)),
            pltpu.SemaphoreType.DMA((16,)),
        ],
        compiler_params=pltpu.CompilerParams(vmem_limit_bytes=16 * MIB),
        cost_estimate=cost(8 * TOK * D * COLS, 1),
        name="first",
    )(*[pltpu.with_memory_space_constraint(v, pltpu.HBM) for v in (x, w, up, hc, lag)])


RESTS = tuple((g, k) for k in (1, 2, 3) for g in range(2))


def rest_kernel(dg_ref, xt_ref, lag_ref, ss_in, *outs):
    ss_ref = outs[-1]
    ss_ref[...] = ss_in[...]
    for s, (g, k) in enumerate(RESTS):
        change_of(g, k, dg_ref, xt_ref, lag_ref, ss_ref, outs[2 * s : 2 * s + 2])


def rest(dg, xt, lag, ss):
    return pl.pallas_call(
        rest_kernel,
        in_specs=[VMEM] * 4,
        out_specs=[VMEM] * 13,
        out_shape=[shape(*PIECE)] * 12 + [shape(8, 128, dtype=jnp.float32)],
        compiler_params=pltpu.CompilerParams(vmem_limit_bytes=10 * MIB),
        cost_estimate=cost(2 * TOK * D * COLS, 20_000_000),
        name="rest",
    )(dg, xt, lag, ss)


def input_part(w_ref, dg_ref, z, c):
    row = pl.multiple_of((z * 2 + c) * INB, 64)
    return lax.dot_general(
        w_ref[pl.ds(row, INB), :],
        dg_ref[...],
        (((1,), (1,)), ((), ())),
        preferred_element_type=jnp.float32,
    )


def z_order():
    z = lax.axis_index("z")
    return (z + 1) % 4, (z + 3) % 4, (z + 2) % 4, z


def away_kernel(w_ref, dg_ref, out_ref):
    c = 1 - lax.axis_index("c")
    for i, z in enumerate(z_order()):
        out_ref[i] = bf16(input_part(w_ref, dg_ref, z, c))


def mine_kernel(w_ref, dg_ref, got_ref, *outs):
    c = lax.axis_index("c")
    for i, z in enumerate(z_order()):
        outs[i][...] = bf16(input_part(w_ref, dg_ref, z, c) + f32(got_ref[i]))


def local(kernel, out_shape, *args, limit=8, flops=1_000_000, specs=None):
    single = not isinstance(out_shape, list)
    return pl.pallas_call(
        kernel,
        in_specs=specs or [VMEM] * len(args),
        out_specs=VMEM if single else [VMEM] * len(out_shape),
        out_shape=out_shape,
        compiler_params=pltpu.CompilerParams(vmem_limit_bytes=limit * MIB),
        cost_estimate=cost(flops, 1_000_000),
    )(*args)


def factor_kernel(mask_ref, total_ref, factor_ref, rms_ref):
    total = jnp.sum(total_ref[...], axis=(0, 1), keepdims=True)
    rms = jnp.sqrt(total / (D * FF) + 1e-06)
    factor = f32(mask_ref[0]) * jnp.minimum(1.0, CLIP / rms)
    factor_ref[...] = jnp.broadcast_to(factor, (8, 128))
    rms_ref[...] = jnp.broadcast_to(rms, (8, 128))


def one(ref):
    return ref[0:1, 0:1]


def mixed_kernel(own_f, *refs):
    theirs, far, relay, outs = refs[0:4], refs[4:8], refs[8:12], refs[12:16]
    for p in range(4):
        for m in range(4):
            outs[p][m] = bf16(one(own_f) * f32(far[p][m]) + one(theirs[p]) * f32(relay[p][m]))


def merged(own_f, their_f, own, near, far, m):
    return one(own_f) * f32(own[m]) + one(their_f) * f32(near[m]) + f32(far[m])


def third_kernel(own_f, *refs):
    theirs, own, near, far, outs = (refs[4 * i : 4 * i + 4] for i in range(5))
    for p, (g, h) in enumerate(PARTS):
        for m in range(2):
            outs[p][m] = bf16(merged(own_f, theirs[p], own[p], near[p], far[p], h + m))


def fourth_kernel(own_f, *refs):
    theirs, own, near, far, third, outs = (refs[4 * i : 4 * i + 4] for i in range(6))
    for p, (g, h) in enumerate(PARTS):
        value = merged(own_f, theirs[p], own[p], near[p], far[p], 2 - 2 * h)
        outs[p][0] = bf16(value + f32(third[p][1 - h]))


def final_kernel(own_f, agg_ref, *refs):
    theirs, own, near, far, third, fourth = (refs[4 * i : 4 * i + 4] for i in range(6))
    out_ref = refs[24]
    for p, (g, h) in enumerate(PARTS):
        value = merged(own_f, theirs[p], own[p], near[p], far[p], 3)
        at = (slice(h * SUB, (h + 1) * SUB), slice(g * HALF, (g + 1) * HALF))
        out_ref[at] = agg_ref[at] + (value + f32(third[p][h]) + f32(fourth[p][0]))


def inputs_kernel(mine_ref, a_ref, b_ref, c_ref, out_ref):
    out_ref[...] = bf16(f32(mine_ref[...]) + f32(a_ref[...]) + f32(b_ref[...]) + f32(c_ref[...]))


def swap(value, axis, pairs):
    return lax.ppermute(value, axis, pairs)


def body(tokens, gate_weight, up_act, hidden_cot, lag_grads, skip_mask, aggregate):
    dg, xt, w, lag, *relay, ss = first(
        tokens, gate_weight, up_act, hidden_cot, lag_grads[0]
    )
    got_relay = [swap(relay[2 * g + h], AXES[g][0], PAIRS[h]) for g, h in PARTS]
    *pieces, total = rest(dg, xt, lag, ss)
    piece = {}
    for s, (g, k) in enumerate(RESTS):
        for h in range(2):
            piece[g, k, h] = pieces[2 * s + h]
    got_near = [swap(piece[g, 1 + h, h], AXES[g][0], PAIRS[h]) for g, h in PARTS]
    total = total + swap(total, "c", [(0, 1), (1, 0)])
    total = total + swap(total, "z", EVEN)
    total = total + swap(total, "z", ODD)
    small = shape(8, 128, dtype=jnp.float32)
    factor, rms = local(
        factor_kernel, [small, small], skip_mask, total, specs=[SMEM, VMEM], limit=1
    )
    theirs = [swap(factor, AXES[g][0], PAIRS[h]) for g, h in PARTS]

    flops = TOK * D * COLS
    away = local(away_kernel, shape(4, INB, TOK), w, dg, flops=flops, limit=4)
    away = swap(away, "c", [(0, 1), (1, 0)])
    up1, down1, two, mine = local(
        mine_kernel, [shape(INB, TOK)] * 4, w, dg, away, flops=flops, limit=4
    )
    ring = lambda by: [(i, (i + by) % 4) for i in range(4)]
    moved = [swap(up1, "z", ring(1)), swap(down1, "z", ring(3)), swap(two, "z", ring(2))]
    inp = local(inputs_kernel, shape(INB, TOK), mine, *moved)

    mixed = local(
        mixed_kernel, [shape(*PIECE)] * 4,
        factor, *theirs, *[piece[g, 2 - h, h] for g, h in PARTS], *got_relay,
    )
    got_far = [swap(value, AXES[g][0], PAIRS[1 - h]) for (g, h), value in zip(PARTS, mixed)]
    known = [*theirs, *[piece[g, 3, h] for g, h in PARTS], *got_near, *got_far]
    third = local(third_kernel, [shape(2, SUB, HALF)] * 4, factor, *known)
    third = [swap(v, AXES[g][1], PAIRS[h]) for (g, h), v in zip(PARTS, third)]
    fourth = local(fourth_kernel, [shape(1, SUB, HALF)] * 4, factor, *known, *third)
    fourth = [swap(v, AXES[g][1], PAIRS[1 - h]) for (g, h), v in zip(PARTS, fourth)]
    new = local(
        final_kernel, shape(BLK, COLS, dtype=jnp.float32),
        factor, aggregate, *known, *third, *fourth,
    )
    return new, inp.T, rms[0, :1]


def solution(mesh):
    finer = Mesh(mesh.devices.reshape(4, 4, 4, 2), ("y", "x", "z", "c"))
    dp = ("y", "x")
    placed = (
        P(dp, None),
        P(None, TENSOR),
        P(dp, TENSOR),
        P(dp, TENSOR),
        P(dp, None, TENSOR),
        P(dp),
        P(dp, TENSOR),
    )
    return jax.shard_map(
        body,
        mesh=finer,
        in_specs=placed,
        out_specs=(P(dp, TENSOR), P(dp, TENSOR), P(dp)),
        check_vma=False,
    )
```
